64 devices in a mesh: data: 4 (over x, y), ctx: 16 (over z, core).
Axes of the slice: x: 2, y: 2, z: 8, core: 2. Of those that a mesh axis runs over, the one named last changes fastest.
The devices are a block of a 4x4x8 slice.
Arguments:
- queries: bfloat16 [4, 8192, 16, 128], P('data', 'ctx'), parts along dimension 0
- keys_in: bfloat16 [4, 8192, 4, 128], P('data', 'ctx'), parts along dimension 0
- values_in: bfloat16 [4, 8192, 4, 128], P('data', 'ctx'), parts along dimension 0
- grad_out: bfloat16 [4, 8192, 16, 128], P('data', 'ctx'), parts along dimension 0
Outputs:
- output 1: bfloat16 [4, 8192, 16, 128], P('data', 'ctx'), parts along dimension 0
- output 2: bfloat16 [4, 8192, 16, 128], P('data', 'ctx'), parts along dimension 0
- output 3: bfloat16 [4, 8192, 4, 128], P('data', 'ctx'), parts along dimension 0
- output 4: bfloat16 [4, 8192, 4, 128], P('data', 'ctx'), parts along dimension 0
There are 4 independent parts. The reference program is written for one: setup_inputs(seed, part) draws one part's arguments, and reference() takes and returns one part's arrays. A program takes and returns all parts, laid end to end along the dimension named above; each array names one.
All inputs are finite; a program needn't handle non-finite values.
Results may differ from the reference program's by a relative error of at most 0.0169614.
Values are sent between devices in bfloat16 or wider.
A program may use at most 768 MiB of HBM per device.

```python
import jax
import jax.numpy as jnp
from jax import lax

BATCH = 1
TOKENS_DEV = 512
CTX_DEVICES = 16
Q_LOCAL = 16
KV_LOCAL = 4
HEAD_DIM = 128

SEQ_LEN = CTX_DEVICES * TOKENS_DEV
HALF_LEN = TOKENS_DEV // 2
NUM_PIECES = 2 * CTX_DEVICES
GROUP_SIZE = Q_LOCAL // KV_LOCAL
SPREAD = 1.6


def true_positions():
    token_index = jnp.arange(SEQ_LEN, dtype=jnp.int32)
    shard_id = token_index // TOKENS_DEV
    offset = token_index % TOKENS_DEV
    low_pos = shard_id * HALF_LEN + offset
    high_pos = (NUM_PIECES - 1 - shard_id) * HALF_LEN + offset - HALF_LEN
    return jnp.where(offset < HALF_LEN, low_pos, high_pos)


def setup_inputs(seed: int = 0, part: int = 0) -> dict:
    base_key = jax.random.fold_in(jax.random.key(seed), part)
    key_q, key_k, key_v, key_g = jax.random.split(base_key, 4)
    q_shape = (BATCH, SEQ_LEN, Q_LOCAL, HEAD_DIM)
    kv_shape = (BATCH, SEQ_LEN, KV_LOCAL, HEAD_DIM)
    queries = SPREAD * jax.random.normal(key_q, q_shape, jnp.float32)
    keys_in = SPREAD * jax.random.normal(key_k, kv_shape, jnp.float32)
    values_in = jax.random.normal(key_v, kv_shape, jnp.float32)
    grad_out = jax.random.normal(key_g, q_shape, jnp.float32)
    return {"queries": queries.astype(jnp.bfloat16), "keys_in": keys_in.astype(jnp.bfloat16), "values_in": values_in.astype(jnp.bfloat16), "grad_out": grad_out.astype(jnp.bfloat16)}


def reference(queries, keys_in, values_in, grad_out):
    score_scale = HEAD_DIM ** -0.5
    positions = true_positions()
    block_pos = positions.reshape(NUM_PIECES, HALF_LEN)
    keys_wide = keys_in.astype(jnp.float32)
    values_wide = values_in.astype(jnp.float32)

    def to_blocks(tensor):
        return tensor.reshape(BATCH, NUM_PIECES, HALF_LEN, KV_LOCAL, GROUP_SIZE, HEAD_DIM).transpose(1, 0, 2, 3, 4, 5)

    def from_blocks(tensor):
        return tensor.transpose(1, 0, 2, 3, 4, 5).reshape(BATCH, SEQ_LEN, Q_LOCAL, HEAD_DIM)

    def masked_scores(q_blk, pos_blk):
        raw_scores = jnp.einsum("bqhgd,bkhd->bhgqk", q_blk.astype(jnp.float32), keys_wide) * score_scale
        visible = pos_blk[:, None] >= positions[None, :]
        return jnp.where(visible, raw_scores, -jnp.inf)

    def forward_block(blk_args):
        q_blk, pos_blk = blk_args
        masked = masked_scores(q_blk, pos_blk)
        row_max = jnp.max(masked, axis=-1)
        row_sum = jnp.sum(jnp.exp(masked - row_max[..., None]), axis=-1)
        log_sum = row_max + jnp.log(row_sum)
        prob_tile = jnp.exp(masked - log_sum[..., None]).astype(jnp.bfloat16).astype(jnp.float32)
        out_blk = jnp.einsum("bhgqk,bkhd->bqhgd", prob_tile, values_wide)
        return out_blk.astype(jnp.bfloat16), log_sum

    q_blocks = to_blocks(queries)
    g_blocks = to_blocks(grad_out)
    out_blocks, lse_blocks = lax.map(forward_block, (q_blocks, block_pos))
    d_rows = jnp.einsum("nbqhgd,nbqhgd->nbhgq", g_blocks.astype(jnp.float32), out_blocks.astype(jnp.float32))

    def backward_step(loop_carry, blk_args):
        dk_acc, dv_acc = loop_carry
        q_blk, g_blk, lse_blk, drow_blk, pos_blk = blk_args
        q_wide = q_blk.astype(jnp.float32)
        g_wide = g_blk.astype(jnp.float32)
        prob_tile = jnp.exp(masked_scores(q_blk, pos_blk) - lse_blk[..., None])
        prob_low = prob_tile.astype(jnp.bfloat16).astype(jnp.float32)
        dv_acc = dv_acc + jnp.einsum("bhgqk,bqhgd->bkhd", prob_low, g_wide)
        dprob_tile = jnp.einsum("bqhgd,bkhd->bhgqk", g_wide, values_wide)
        dscore_tile = (prob_tile * (dprob_tile - drow_blk[..., None])).astype(jnp.bfloat16).astype(jnp.float32)
        dq_blk = jnp.einsum("bhgqk,bkhd->bqhgd", dscore_tile, keys_wide) * score_scale
        dk_acc = dk_acc + jnp.einsum("bhgqk,bqhgd->bkhd", dscore_tile, q_wide) * score_scale
        return (dk_acc, dv_acc), dq_blk.astype(jnp.bfloat16)

    zeros_kv = jnp.zeros((BATCH, SEQ_LEN, KV_LOCAL, HEAD_DIM), jnp.float32)
    grads_kv, dq_blocks = lax.scan(backward_step, (zeros_kv, zeros_kv), (q_blocks, g_blocks, lse_blocks, d_rows, block_pos))
    return (from_blocks(out_blocks), from_blocks(dq_blocks), grads_kv[0].astype(jnp.bfloat16), grads_kv[1].astype(jnp.bfloat16))
```

```python
import functools
import math

import jax
import jax.numpy as jnp
from jax import lax
from jax.experimental import pallas as pl
from jax.experimental.pallas import tpu as pltpu
from jax.sharding import PartitionSpec as P

F32 = jnp.float32
BF16 = jnp.bfloat16
NEG = -1e30
MESH = pl.DeviceIdType.MESH
NT_DIMS = (((1,), (1,)), ((), ()))


def dot(a, b):
    return jnp.dot(a, b, preferred_element_type=F32)


def dot_nt(a, b):
    return lax.dot_general(a, b, NT_DIMS, preferred_element_type=F32)


def attention_kernel(
    chips, q_in, k_in, v_in, g_in, o_out, dq_out, dk_out, dv_out,
    qn, gn, kvb, oT, ms, ls, ob, rbuf, acc, dkb,
    in_loc, in_send, in_recv, ag_send, ag_recv, rs_send, rs_recv, out_loc, out_send, out_recv,
):
    q_mine = qn.shape[0]
    piece, dim = qn.shape[3], qn.shape[4]
    kv_mine = kvb.shape[1]
    group = q_mine // kv_mine
    half = chips // 2
    scale = dim ** -0.5
    cexp = scale * math.log2(math.e)
    keys = 2 * piece

    me = lax.axis_index("ctx")
    core = me % 2
    chip = me // 2
    other = 1 - core
    n_dev = 2 * chips
    partner = me + 1 - 2 * core
    up = (me + 2) % n_dev
    down = (me + n_dev - 2) % n_dev

    barrier = pltpu.get_barrier_semaphore()
    for neighbour in (partner, up, down):
        pl.semaphore_signal(barrier, inc=1, device_id={"ctx": neighbour}, device_id_type=MESH)
    pl.semaphore_wait(barrier, 3)

    kv_at = lambda ref, core_id: ref.at[pl.ds(kv_mine * core_id, kv_mine)]
    q_at = lambda ref, core_id: ref.at[pl.ds(q_mine * core_id, q_mine)]

    ins = (
        (k_in, kv_at, kvb.at[chip, :, 0, :, core]),
        (v_in, kv_at, kvb.at[chip, :, 1, :, core]),
        (q_in, q_at, qn.at[:, :, core]),
        (g_in, q_at, gn.at[:, :, core]),
    )

    def in_copies(n):
        src, at, dst = ins[n]
        local = pltpu.make_async_copy(at(src, core), dst, in_loc.at[n])
        remote = pltpu.make_async_remote_copy(
            src_ref=at(src, other), dst_ref=dst, send_sem=in_send.at[n], recv_sem=in_recv.at[n],
            device_id={"ctx": partner}, device_id_type=MESH)
        return local, remote

    def wait_in(n):
        local, remote = in_copies(n)
        local.wait()
        remote.wait()

    for n in range(4):
        local, remote = in_copies(n)
        local.start()
        remote.start()

    def ring_to(direction):
        return (me + n_dev + 2 - 4 * direction) % n_dev

    def ag_copy(b, h, direction, hop):
        return pltpu.make_async_remote_copy(
            src_ref=kvb.at[b, h], dst_ref=kvb.at[b, h],
            send_sem=ag_send.at[direction, h, hop - 1], recv_sem=ag_recv.at[direction, h, hop - 1],
            device_id={"ctx": ring_to(direction)}, device_id_type=MESH)

    def item(t):
        r = t % 4
        h = ((r + 1) // 2) % 2
        return t // 4, r, h, r % 2

    n_items = 4 * half - 2

    wait_in(0)
    wait_in(1)
    for r in range(4):
        ag_copy(chip, ((r + 1) // 2) % 2, r % 2, 1).start()

    def init_body(n, carry):
        gi, qc = n // 4, n % 4
        ms[gi, qc] = jnp.full((1, piece), NEG, F32)
        ls[gi, qc] = jnp.zeros((1, piece), F32)
        oT[gi, qc] = jnp.zeros((dim, piece), F32)
        return carry

    lax.fori_loop(0, q_mine * 4, init_body, 0)
    wait_in(2)
    wait_in(3)

    def visible(x, qc, width):
        k_idx = lax.broadcasted_iota(jnp.int32, (keys, width), 0)
        q_idx = lax.broadcasted_iota(jnp.int32, (keys, width), 1)
        if width > piece:
            q_idx = q_idx % piece
        in_high = (k_idx >= piece).astype(jnp.int32)
        k_pos = k_idx + x * (piece - keys * in_high)
        q_pos = q_idx + (piece * qc + x * (piece * (3 - 2 * qc)))
        return k_pos <= q_pos

    def fwd_step(b, h, x, qc, own):
        hi, co = qc // 2, qc % 2
        kk = kvb[b, h, 0, x].reshape(keys, dim)
        vv = kvb[b, h, 1, x].reshape(keys, dim)
        heads = [h * group + g for g in range(group)]
        q = jnp.concatenate([qn[gi, hi, co] for gi in heads], axis=0)
        s = dot_nt(kk, q)
        if own:
            s = jnp.where(visible(x, qc, group * piece), s, NEG)
        m0 = jnp.concatenate([ms[gi, qc] for gi in heads], axis=1)
        l0 = jnp.concatenate([ls[gi, qc] for gi in heads], axis=1)
        m1 = jnp.maximum(m0, jnp.max(s, axis=0, keepdims=True))
        p = jnp.exp2((s - m1) * cexp)
        decay = jnp.exp2((m0 - m1) * cexp)
        l1 = l0 * decay + jnp.sum(p, axis=0, keepdims=True)
        pv = dot(vv.T, p.astype(BF16))
        for g, gi in enumerate(heads):
            cols = slice(g * piece, (g + 1) * piece)
            ms[gi, qc] = m1[:, cols]
            ls[gi, qc] = l1[:, cols]
            oT[gi, qc] = oT[gi, qc] * decay[:, cols] + pv[:, cols]

    def bwd_step(b, h, x, qc, slot, own):
        hi, co = qc // 2, qc % 2
        kk = kvb[b, h, 0, x].reshape(keys, dim)
        vv = kvb[b, h, 1, x].reshape(keys, dim)
        k_t = kk.T
        mask = visible(x, qc, piece) if own else None
        dv = dk = None
        for g in range(group):
            gi = h * group + g
            q = qn[gi, hi, co]
            do = gn[gi, hi, co]
            s = dot_nt(kk, q)
            if own:
                s = jnp.where(mask, s, NEG)
            p = jnp.exp2(s * cexp - ms[gi, qc])
            dp = dot_nt(vv, do)
            ds = (p * (dp - ls[gi, qc])).astype(BF16)
            dv_part = dot(p.astype(BF16), do)
            dk_part = dot(ds, q)
            dv = dv_part if dv is None else dv + dv_part
            dk = dk_part if dk is None else dk + dk_part
            oT[gi, qc] += dot(k_t, ds)
        acc[slot, 0, x] += dk.reshape(2, piece, dim)
        acc[slot, 1, x] += dv.reshape(2, piece, dim)

    def far_steps(b, step):
        past = (b < chip).astype(jnp.int32)

        def body(w, carry):
            x = (1 - past) * (w // 2)
            qc = past * w + (1 - past) * (2 + w % 2)
            step(x, qc)
            return carry

        lax.fori_loop(0, 4, body, 0)

    def own_steps(step):
        def body(n, carry):
            x = n // 4
            step(x, n - 2 * x)
            return carry

        lax.fori_loop(0, 6, body, 0)

    def own_fwd(h, carry):
        own_steps(lambda x, qc: fwd_step(chip, h, x, qc, True))
        return carry

    lax.fori_loop(0, kv_mine, own_fwd, 0)

    def fwd_item(t, carry):
        j, r, h, direction = item(t)
        d = j + 1
        b = (chip + chips + (2 * direction - 1) * d) % chips
        ag_copy(b, h, direction, d).wait_recv()

        @pl.when(d < half - r // 2)
        def _():
            ag_copy(b, h, direction, d + 1).start()

        far_steps(b, lambda x, qc: fwd_step(b, h, x, qc, False))
        return carry

    lax.fori_loop(0, n_items, fwd_item, 0)

    def fwd_end(n, carry):
        gi, qc = n // 4, n % 4
        hi, co = qc // 2, qc % 2
        total = ls[gi, qc]
        o_t = oT[gi, qc] / total
        ob[gi, hi, co] = o_t.T.astype(BF16)
        do_t = gn[gi, hi, co].astype(F32).T
        ls[gi, qc] = jnp.sum(o_t.astype(BF16).astype(F32) * do_t, axis=0, keepdims=True)
        ms[gi, qc] = ms[gi, qc] * cexp + jnp.log(total) * math.log2(math.e)
        oT[gi, qc] = jnp.zeros((dim, piece), F32)
        return carry

    lax.fori_loop(0, q_mine * 4, fwd_end, 0)

    outs = (
        (o_out, q_at, lambda k: ob.at[:, :, k]),
        (dq_out, q_at, lambda k: ob.at[:, :, k]),
        (dk_out, kv_at, lambda k: dkb.at[0, :, :, k]),
        (dv_out, kv_at, lambda k: dkb.at[1, :, :, k]),
    )

    def out_copies(n):
        dst, at, src = outs[n]
        local = pltpu.make_async_copy(src(core), at(dst, core), out_loc.at[n])
        remote = pltpu.make_async_remote_copy(
            src_ref=src(other), dst_ref=at(dst, core), send_sem=out_send.at[n], recv_sem=out_recv.at[n],
            device_id={"ctx": partner}, device_id_type=MESH)
        return local, remote

    def start_out(n):
        local, remote = out_copies(n)
        local.start()
        remote.start()

    start_out(0)

    def rs_copy(b, h, direction, d, slot):
        return pltpu.make_async_remote_copy(
            src_ref=rbuf.at[b, h], dst_ref=rbuf.at[slot, h],
            send_sem=rs_send.at[direction, h, d - 1], recv_sem=rs_recv.at[direction, h, d - 1],
            device_id={"ctx": ring_to(1 - direction)}, device_id_type=MESH)

    def rs_item(t):
        j, r, h, direction = item(t)
        d = half - r // 2 - j
        b = (chip + chips + (2 * direction - 1) * d) % chips
        last = (d == 1).astype(jnp.int32)
        slot = b + last * direction * (chips - b)
        return j, h, direction, d, b, slot

    def bwd_item(t, carry):
        j, h, direction, d, b, slot = rs_item(t)
        acc[0] = jnp.zeros(acc.shape[1:], F32)
        far_steps(b, lambda x, qc: bwd_step(b, h, x, qc, 0, False))

        @pl.when(j == 0)
        def _():
            rbuf[b, h] = acc[0]

        @pl.when(j > 0)
        def _():
            rs_copy(b, h, direction, d + 1, b).wait_recv()
            rbuf[b, h] += acc[0]

        rs_copy(b, h, direction, d, slot).start()
        return carry

    lax.fori_loop(0, n_items, bwd_item, 0)

    def own_bwd(h, carry):
        acc[h] = jnp.zeros(acc.shape[1:], F32)
        own_steps(lambda x, qc: bwd_step(chip, h, x, qc, h, True))
        return carry

    lax.fori_loop(0, kv_mine, own_bwd, 0)

    def wait_out(n, received):
        local, remote = out_copies(n)
        local.wait()
        remote.wait_send()
        if received:
            remote.wait_recv()

    wait_out(0, True)

    def dq_end(n, carry):
        gi, qc = n // 4, n % 4
        ob[gi, qc // 2, qc % 2] = (oT[gi, qc] * scale).T.astype(BF16)
        return carry

    lax.fori_loop(0, q_mine * 4, dq_end, 0)
    start_out(1)

    def kv_end(h, carry):
        for direction in range(2):
            rs_copy(chip, h, direction, 1, chip).wait_recv()
        for kv in range(2):
            total = acc[h, kv] + rbuf[chip, h, kv] + rbuf[chips, h, kv]
            if kv == 0:
                total = total * scale
            dkb[kv, h] = total.astype(BF16)
        return carry

    lax.fori_loop(0, kv_mine, kv_end, 0)
    start_out(2)
    start_out(3)

    def drain(t, carry):
        j, h, direction, d, b, slot = rs_item(t)
        rs_copy(b, h, direction, d, slot).wait_send()
        return carry

    lax.fori_loop(0, n_items, drain, 0)

    def drain_ag(t, carry):
        j, r, h, direction = item(t)
        b = (chip + chips + (2 * direction - 1) * j) % chips
        ag_copy(b, h, direction, j + 1).wait_send()
        return carry

    lax.fori_loop(0, n_items, drain_ag, 0)
    for n in range(1, 4):
        wait_out(n, True)


def solution(mesh):
    chips = mesh.shape["ctx"] // 2
    block_spec = P("data", "ctx", None, None)

    def heads_first(x):
        _, tokens, heads, dim = x.shape
        return jnp.transpose(x[0], (1, 0, 2)).reshape(heads, 2, tokens // 2, dim)

    def tokens_first(x, like):
        _, tokens, heads, dim = like.shape
        return jnp.transpose(x.reshape(heads, tokens, dim), (1, 0, 2))[None]

    def local_attention(queries, keys_in, values_in, grad_out):
        _, tokens, q_heads, dim = queries.shape
        kv_heads = keys_in.shape[2]
        piece = tokens // 2
        q_mine, kv_mine = q_heads // 2, kv_heads // 2
        half = chips // 2
        dma = pltpu.SemaphoreType.DMA
        q_shape = jax.ShapeDtypeStruct((q_heads, 2, piece, dim), BF16)
        kv_shape = jax.ShapeDtypeStruct((kv_heads, 2, piece, dim), BF16)
        any_spec = pl.BlockSpec(memory_space=pl.ANY)
        outs = pl.pallas_call(
            functools.partial(attention_kernel, chips),
            out_shape=(q_shape, q_shape, kv_shape, kv_shape),
            in_specs=[any_spec] * 4,
            out_specs=(any_spec,) * 4,
            scratch_shapes=[
                pltpu.VMEM((q_mine, 2, 2, piece, dim), BF16),
                pltpu.VMEM((q_mine, 2, 2, piece, dim), BF16),
                pltpu.VMEM((chips, kv_mine, 2, 2, 2, piece, dim), BF16),
                pltpu.VMEM((q_mine, 4, dim, piece), F32),
                pltpu.VMEM((q_mine, 4, 1, piece), F32),
                pltpu.VMEM((q_mine, 4, 1, piece), F32),
                pltpu.VMEM((q_mine, 2, 2, piece, dim), BF16),
                pltpu.VMEM((chips + 1, kv_mine, 2, 2, 2, piece, dim), F32),
                pltpu.VMEM((kv_mine, 2, 2, 2, piece, dim), F32),
                pltpu.VMEM((2, kv_mine, 2, 2, piece, dim), BF16),
                dma((4,)), dma((4,)), dma((4,)),
                dma((2, kv_mine, half)), dma((2, kv_mine, half)),
                dma((2, kv_mine, half)), dma((2, kv_mine, half)),
                dma((4,)), dma((4,)), dma((4,)),
            ],
            compiler_params=pltpu.CompilerParams(
                collective_id=0, has_side_effects=True, vmem_limit_bytes=60 * 2**20),
            name="ring_attention",
        )(heads_first(queries), heads_first(keys_in), heads_first(values_in), heads_first(grad_out))
        likes = (queries, queries, keys_in, keys_in)
        return tuple(tokens_first(x, like) for x, like in zip(outs, likes))

    return jax.shard_map(local_attention, mesh=mesh, in_specs=(block_spec,) * 4, out_specs=(block_spec,) * 4, check_vma=False)
```

```python
import functools
import math

import jax
import jax.numpy as jnp
from jax import lax
from jax.experimental import pallas as pl
from jax.experimental.pallas import tpu as pltpu
from jax.sharding import PartitionSpec as P

F32 = jnp.float32
BF16 = jnp.bfloat16
NEG = -1e30
MESH = pl.DeviceIdType.MESH
NT_DIMS = (((1,), (1,)), ((), ()))


def dot(a, b):
    return jnp.dot(a, b, preferred_element_type=F32)


def dot_nt(a, b):
    return lax.dot_general(a, b, NT_DIMS, preferred_element_type=F32)


def attention_kernel(
    chips, q_in, k_in, v_in, g_in, o_out, dq_out, dk_out, dv_out,
    qn, gn, kvb, oT, ms, ls, raw, rawf, rbuf, acc, dkb,
    in_loc, in_send, in_recv, ag_send, ag_recv, rs_send, rs_recv, out_loc, out_send, out_recv,
):
    q_mine = qn.shape[0]
    piece, dim = qn.shape[3], qn.shape[4]
    kv_mine = kvb.shape[1]
    group = q_mine // kv_mine
    half = chips // 2
    scale = dim ** -0.5
    cexp = scale * math.log2(math.e)
    keys = 2 * piece

    me = lax.axis_index("ctx")
    core = me % 2
    chip = me // 2
    other = 1 - core
    n_dev = 2 * chips
    partner = me + 1 - 2 * core
    up = (me + 2) % n_dev
    down = (me + n_dev - 2) % n_dev

    barrier = pltpu.get_barrier_semaphore()
    for neighbour in (partner, up, down):
        pl.semaphore_signal(barrier, inc=1, device_id={"ctx": neighbour}, device_id_type=MESH)
    pl.semaphore_wait(barrier, 3)

    kv_at = lambda ref, core_id: ref.at[pl.ds(kv_mine * core_id, kv_mine)]
    q_at = lambda ref, core_id: ref.at[:, :, core_id]

    ins = (
        (k_in, kv_at, kvb.at[chip, :, 0, :, core]),
        (v_in, kv_at, kvb.at[chip, :, 1, :, core]),
        (q_in, q_at, raw.at[0, :, core]),
        (g_in, q_at, raw.at[1, :, core]),
    )

    def in_copies(n):
        src, at, dst = ins[n]
        local = pltpu.make_async_copy(at(src, core), dst, in_loc.at[n])
        remote = pltpu.make_async_remote_copy(
            src_ref=at(src, other), dst_ref=dst, send_sem=in_send.at[n], recv_sem=in_recv.at[n],
            device_id={"ctx": partner}, device_id_type=MESH)
        return local, remote

    def wait_in(n):
        local, remote = in_copies(n)
        local.wait()
        remote.wait()

    for n in range(4):
        local, remote = in_copies(n)
        local.start()
        remote.start()

    def ring_to(direction):
        return (me + n_dev + 2 - 4 * direction) % n_dev

    def ag_copy(b, h, direction, hop, kv):
        return pltpu.make_async_remote_copy(
            src_ref=kvb.at[b, h, kv], dst_ref=kvb.at[b, h, kv],
            send_sem=ag_send.at[direction, h, hop - 1, kv], recv_sem=ag_recv.at[direction, h, hop - 1, kv],
            device_id={"ctx": ring_to(direction)}, device_id_type=MESH)

    def chain_of(name):
        return {"A": (0, 0), "D": (0, 1), "C": (1, 0), "B": (1, 1)}[name]

    def pick(n, values):
        if len(set(values)) == 1:
            return values[0]
        total = 0
        for k, value in enumerate(values):
            if value:
                total = total + value * (n == k).astype(jnp.int32)
        return total

    def pick_item(n, names):
        chains = [chain_of(name[0]) for name in names]
        h = pick(n, [c[0] for c in chains])
        direction = pick(n, [c[1] for c in chains])
        return h, direction, pick(n, [int(name[1:]) for name in names])

    def owner(direction, d):
        return (chip + chips + (2 * direction - 1) * d) % chips

    def receive(h, direction, d, hold=False):
        b = owner(direction, d)
        hops = half - (h + direction) % 2
        for kv in range(2):
            ag_copy(b, h, direction, d, kv).wait_recv()

            @pl.when((d < hops) & jnp.logical_not(hold))
            def _():
                ag_copy(b, h, direction, d + 1, kv).start()

    wait_in(0)
    wait_in(1)
    for name in "AD":
        for kv in range(2):
            ag_copy(chip, *chain_of(name), 1, kv).start()

    def init_body(n, carry):
        gi, qc = n // 4, n % 4
        ms[gi, qc] = jnp.full((1, piece), NEG, F32)
        ls[gi, qc] = jnp.zeros((1, piece), F32)
        oT[gi, qc] = jnp.zeros((dim, piece), F32)
        return carry

    lax.fori_loop(0, q_mine * 4, init_body, 0)

    def split_heads(n, dst):
        def body(c, carry):
            hi, co = c // 2, c % 2
            rawf[c] = raw[n, hi, co].astype(F32).reshape(piece * q_mine, dim)
            for gi in range(q_mine):
                dst[gi, hi, co] = rawf[c, pl.ds(gi, piece, stride=q_mine), :].astype(BF16)
            return carry

        wait_in(2 + n)
        lax.fori_loop(0, 4, body, 0)

    def join_heads(n):
        def body(c, carry):
            raw[n, c // 2, c % 2] = rawf[c].reshape(piece, q_mine, dim).astype(BF16)
            return carry

        lax.fori_loop(0, 4, body, 0)

    split_heads(0, qn)

    def visible(x, qc, width):
        k_idx = lax.broadcasted_iota(jnp.int32, (keys, width), 0)
        q_idx = lax.broadcasted_iota(jnp.int32, (keys, width), 1)
        if width > piece:
            q_idx = q_idx % piece
        in_high = (k_idx >= piece).astype(jnp.int32)
        k_pos = k_idx + x * (piece - keys * in_high)
        q_pos = q_idx + (piece * qc + x * (piece * (3 - 2 * qc)))
        return k_pos <= q_pos

    def fwd_step(b, h, x, qc, own):
        hi, co = qc // 2, qc % 2
        kk = kvb[b, h, 0, x].reshape(keys, dim)
        vv = kvb[b, h, 1, x].reshape(keys, dim)
        heads = [h * group + g for g in range(group)]
        q = jnp.concatenate([qn[gi, hi, co] for gi in heads], axis=0)
        s = dot_nt(kk, q)
        if own:
            s = jnp.where(visible(x, qc, group * piece), s, NEG)
        m0 = jnp.concatenate([ms[gi, qc] for gi in heads], axis=1)
        l0 = jnp.concatenate([ls[gi, qc] for gi in heads], axis=1)
        m1 = jnp.maximum(m0, jnp.max(s, axis=0, keepdims=True))
        p = jnp.exp2((s - m1) * cexp)
        decay = jnp.exp2((m0 - m1) * cexp)
        l1 = l0 * decay + jnp.sum(p, axis=0, keepdims=True)
        pv = dot(vv.T, p.astype(BF16))
        for g, gi in enumerate(heads):
            cols = slice(g * piece, (g + 1) * piece)
            ms[gi, qc] = m1[:, cols]
            ls[gi, qc] = l1[:, cols]
            oT[gi, qc] = oT[gi, qc] * decay[:, cols] + pv[:, cols]

    def bwd_step(b, h, x, qc, slot, own):
        hi, co = qc // 2, qc % 2
        kk = kvb[b, h, 0, x].reshape(keys, dim)
        vv = kvb[b, h, 1, x].reshape(keys, dim)
        k_t = kk.T
        mask = visible(x, qc, piece) if own else None
        dv = dk = None
        for g in range(group):
            gi = h * group + g
            q = qn[gi, hi, co]
            do = gn[gi, hi, co]
            s = dot_nt(kk, q)
            if own:
                s = jnp.where(mask, s, NEG)
            p = jnp.exp2(s * cexp - ms[gi, qc])
            dp = dot_nt(vv, do)
            ds = (p * (dp - ls[gi, qc])).astype(BF16)
            dv_part = dot(p.astype(BF16), do)
            dk_part = dot(ds, q)
            dv = dv_part if dv is None else dv + dv_part
            dk = dk_part if dk is None else dk + dk_part
            oT[gi, qc] += dot(k_t, ds)
        acc[slot, 0, x] += dk.reshape(2, piece, dim)
        acc[slot, 1, x] += dv.reshape(2, piece, dim)

    def far_steps(b, step):
        past = (b < chip).astype(jnp.int32)

        def body(w, carry):
            x = (1 - past) * (w // 2)
            qc = past * w + (1 - past) * (2 + w % 2)
            step(x, qc)
            return carry

        lax.fori_loop(0, 4, body, 0)

    def own_steps(step):
        def body(n, carry):
            x = n // 4
            step(x, n - 2 * x)
            return carry

        lax.fori_loop(0, 6, body, 0)

    def own_fwd(h, carry):
        own_steps(lambda x, qc: fwd_step(chip, h, x, qc, True))
        return carry

    lax.fori_loop(0, kv_mine, own_fwd, 0)
    split_heads(1, gn)

    def fwd_far(h, direction, d):
        b = owner(direction, d)
        far_steps(b, lambda x, qc: fwd_step(b, h, x, qc, False))

    first = [f"{c}{d}" for c, d in (("A", 1), ("D", 1), ("A", 2), ("D", 2), ("C", 1), ("B", 1))]
    first += [f"{c}{d}" for d in range(3, half) for c in "AD"] + [f"A{half}", "B2"]

    def fwd_pair(n, carry):
        receive(*pick_item(n, first[0::2]), hold=n == 2)

        @pl.when(n == 3)
        def _():
            for kv in range(2):
                ag_copy(owner(0, 1), *chain_of("C"), 2, kv).start()

        receive(*pick_item(n, first[1::2]))

        @pl.when(n == 0)
        def _():
            for name in "CB":
                for kv in range(2):
                    ag_copy(chip, *chain_of(name), 1, kv).start()

        def one(k, inner):
            fwd_far(*pick_item(2 * n + k, first))
            return inner

        lax.fori_loop(0, 2 - (n == half).astype(jnp.int32), one, 0)
        return carry

    lax.fori_loop(0, half + 1, fwd_pair, 0)

    def fwd_end(h, qc, carry):
        hi, co = qc // 2, qc % 2
        for gi in range(h * group, (h + 1) * group):
            total = ls[gi, qc]
            o_t = oT[gi, qc] / total
            rawf[qc, pl.ds(gi, piece, stride=q_mine), :] = o_t.T
            do_t = gn[gi, hi, co].astype(F32).T
            ls[gi, qc] = jnp.sum(o_t.astype(BF16).astype(F32) * do_t, axis=0, keepdims=True)
            ms[gi, qc] = ms[gi, qc] * cexp + jnp.log(total) * math.log2(math.e)
            oT[gi, qc] = jnp.zeros((dim, piece), F32)
        return carry

    lax.fori_loop(0, 4, functools.partial(fwd_end, 0), 0)

    outs = (
        (o_out, q_at, lambda k: raw.at[0, :, k]),
        (dq_out, q_at, lambda k: raw.at[1, :, k]),
        (dk_out, kv_at, lambda k: dkb.at[0, :, :, k]),
        (dv_out, kv_at, lambda k: dkb.at[1, :, :, k]),
    )

    def out_copies(n):
        dst, at, src = outs[n]
        local = pltpu.make_async_copy(src(core), at(dst, core), out_loc.at[n])
        remote = pltpu.make_async_remote_copy(
            src_ref=src(other), dst_ref=at(dst, core), send_sem=out_send.at[n], recv_sem=out_recv.at[n],
            device_id={"ctx": partner}, device_id_type=MESH)
        return local, remote

    def start_out(n):
        local, remote = out_copies(n)
        local.start()
        remote.start()

    def rs_copy(b, h, direction, d, slot):
        return pltpu.make_async_remote_copy(
            src_ref=rbuf.at[b, h], dst_ref=rbuf.at[slot, h],
            send_sem=rs_send.at[direction, h, d - 1], recv_sem=rs_recv.at[direction, h, d - 1],
            device_id={"ctx": ring_to(1 - direction)}, device_id_type=MESH)

    def rs_send_copy(h, direction, d):
        b = owner(direction, d)
        last = jnp.asarray(d == 1).astype(jnp.int32)
        return rs_copy(b, h, direction, d, b + last * direction * (chips - b))

    def bwd_far(h, direction, d, slot):
        b = owner(direction, d)
        acc[slot] = jnp.zeros(acc.shape[1:], F32)
        far_steps(b, lambda x, qc: bwd_step(b, h, x, qc, slot, False))

    def rs_first(h, direction, d, slot):
        rbuf[owner(direction, d), h] = acc[slot]
        rs_send_copy(h, direction, d).start()

    def rs_next(h, direction, d, slot):
        b = owner(direction, d)
        rs_copy(b, h, direction, d + 1, b).wait_recv()
        rbuf[b, h] += acc[slot]
        rs_send_copy(h, direction, d).start()

    early = [f"A{half}", f"D{half - 1}"]

    def early_item(n, carry):
        which = pick_item(n, early)
        bwd_far(*which, kv_mine)

        @pl.when(n == 0)
        def _():
            receive(*chain_of("C"), 2)
            receive(*chain_of("B"), 3)

        rs_first(*which, kv_mine)
        return carry

    lax.fori_loop(0, 2, early_item, 0)

    second = ["B2", "C2", "B3", "C3", "B4"]

    def fwd_late(n, carry):
        @pl.when(n == 3)
        def _():
            receive(*chain_of("C"), 3)
            receive(*chain_of("B"), 4)

        fwd_far(*pick_item(n, second))
        return carry

    lax.fori_loop(0, len(second), fwd_late, 0)
    lax.fori_loop(0, 4, functools.partial(fwd_end, 1), 0)
    join_heads(0)
    start_out(0)

    late = ["C3", "B4", "A3", "D2", "C2", "B3", "A2", "D1", "C1", "B2"]
    final = ["A1", "B1"]

    def own_bwd(h):
        acc[h] = jnp.zeros(acc.shape[1:], F32)
        own_steps(lambda x, qc: bwd_step(chip, h, x, qc, h, True))

    def late_item(n, carry):
        @pl.when((n == 6) | (n == 8))
        def _():
            own_bwd((n - 6) // 2)

        which = pick_item(n, late + final)
        bwd_far(*which, kv_mine + n // 11)

        @pl.when(n < 2)
        def _():
            rs_first(*which, kv_mine)

        @pl.when((n >= 2) & (n < 10))
        def _():
            rs_next(*which, kv_mine)

        return carry

    lax.fori_loop(0, 12, late_item, 0)

    def wait_out(n):
        local, remote = out_copies(n)
        local.wait()
        remote.wait()

    def dq_end(qc, carry):
        for gi in range(q_mine):
            rawf[qc, pl.ds(gi, piece, stride=q_mine), :] = (oT[gi, qc] * scale).T
        return carry

    lax.fori_loop(0, 4, dq_end, 0)
    join_heads(1)
    start_out(1)

    def final_item(n, carry):
        rs_next(*pick_item(n, final), kv_mine + n)
        return carry

    lax.fori_loop(0, 2, final_item, 0)

    def kv_end(h, carry):
        for direction in range(2):
            rs_copy(chip, h, direction, 1, chip).wait_recv()
        for kv in range(2):
            total = acc[h, kv] + rbuf[chip, h, kv] + rbuf[chips, h, kv]
            if kv == 0:
                total = total * scale
            dkb[kv, h] = total.astype(BF16)
        return carry

    lax.fori_loop(0, kv_mine, kv_end, 0)
    start_out(2)
    start_out(3)

    def drain(n, carry):
        h, direction = n % 2, n // 2
        hops = half - (h + direction) % 2

        def one(d, inner):
            rs_send_copy(h, direction, d).wait_send()
            for kv in range(2):
                ag_copy(owner(direction, d - 1), h, direction, d, kv).wait_send()
            return inner

        lax.fori_loop(1, hops + 1, one, 0)
        return carry

    lax.fori_loop(0, 4, drain, 0)
    for n in range(4):
        wait_out(n)


def solution(mesh):
    chips = mesh.shape["ctx"] // 2
    block_spec = P("data", "ctx", None, None)

    def heads_first(x):
        _, tokens, heads, dim = x.shape
        return jnp.transpose(x[0], (1, 0, 2)).reshape(heads, 2, tokens // 2, dim)

    def token_rows(x):
        _, tokens, heads, dim = x.shape
        return x.reshape(2, tokens // 2, 2, heads // 2, dim)

    def tokens_first(x, like):
        _, tokens, heads, dim = like.shape
        return jnp.transpose(x.reshape(heads, tokens, dim), (1, 0, 2))[None]

    def local_attention(queries, keys_in, values_in, grad_out):
        _, tokens, q_heads, dim = queries.shape
        kv_heads = keys_in.shape[2]
        piece = tokens // 2
        q_mine, kv_mine = q_heads // 2, kv_heads // 2
        half = chips // 2
        dma = pltpu.SemaphoreType.DMA
        q_shape = jax.ShapeDtypeStruct((2, piece, 2, q_mine, dim), BF16)
        kv_shape = jax.ShapeDtypeStruct((kv_heads, 2, piece, dim), BF16)
        any_spec = pl.BlockSpec(memory_space=pl.ANY)
        outs = pl.pallas_call(
            functools.partial(attention_kernel, chips),
            out_shape=(q_shape, q_shape, kv_shape, kv_shape),
            in_specs=[any_spec] * 4,
            out_specs=(any_spec,) * 4,
            scratch_shapes=[
                pltpu.VMEM((q_mine, 2, 2, piece, dim), BF16),
                pltpu.VMEM((q_mine, 2, 2, piece, dim), BF16),
                pltpu.VMEM((chips, kv_mine, 2, 2, 2, piece, dim), BF16),
                pltpu.VMEM((q_mine, 4, dim, piece), F32),
                pltpu.VMEM((q_mine, 4, 1, piece), F32),
                pltpu.VMEM((q_mine, 4, 1, piece), F32),
                pltpu.VMEM((2, 2, 2, piece, q_mine, dim), BF16),
                pltpu.VMEM((4, piece * q_mine, dim), F32),
                pltpu.VMEM((chips + 1, kv_mine, 2, 2, 2, piece, dim), F32),
                pltpu.VMEM((kv_mine + 2, 2, 2, 2, piece, dim), F32),
                pltpu.VMEM((2, kv_mine, 2, 2, piece, dim), BF16),
                dma((4,)), dma((4,)), dma((4,)),
                dma((2, kv_mine, half, 2)), dma((2, kv_mine, half, 2)),
                dma((2, kv_mine, half)), dma((2, kv_mine, half)),
                dma((4,)), dma((4,)), dma((4,)),
            ],
            compiler_params=pltpu.CompilerParams(
                collective_id=0, has_side_effects=True, vmem_limit_bytes=60 * 2**20),
            name="ring_attention",
        )(token_rows(queries), heads_first(keys_in), heads_first(values_in), token_rows(grad_out))
        return (outs[0].reshape(queries.shape), outs[1].reshape(queries.shape),
                tokens_first(outs[2], keys_in), tokens_first(outs[3], keys_in))

    return jax.shard_map(local_attention, mesh=mesh, in_specs=(block_spec,) * 4, out_specs=(block_spec,) * 4, check_vma=False)
```

```python
import functools
import math

import jax
import jax.numpy as jnp
from jax import lax
from jax.experimental import pallas as pl
from jax.experimental.pallas import tpu as pltpu
from jax.sharding import PartitionSpec as P

F32 = jnp.float32
BF16 = jnp.bfloat16
NEG = -1e30
MESH = pl.DeviceIdType.MESH
NT_DIMS = (((1,), (1,)), ((), ()))


def dot(a, b):
    return jnp.dot(a, b, preferred_element_type=F32)


def dot_nt(a, b):
    return lax.dot_general(a, b, NT_DIMS, preferred_element_type=F32)


def attention_kernel(
    chips, q_in, kv_in, g_in, o_out, dq_out, dk_out, dv_out,
    qn, gn, kvb, oT, ms, ls, raw, rawf, rbuf, acc, dkb,
    in_loc, in_send, in_recv, ag_send, ag_recv, rs_send, rs_recv, out_loc, out_send, out_recv,
):
    q_mine = qn.shape[0]
    piece, dim = qn.shape[3], qn.shape[4]
    kv_mine = kvb.shape[1]
    group = q_mine // kv_mine
    half = chips // 2
    scale = dim ** -0.5
    cexp = scale * math.log2(math.e)
    keys = 2 * piece

    me = lax.axis_index("ctx")
    core = me % 2
    chip = me // 2
    other = 1 - core
    n_dev = 2 * chips
    partner = me + 1 - 2 * core
    up = (me + 2) % n_dev
    down = (me + n_dev - 2) % n_dev

    kv_at = lambda ref, core_id: ref.at[pl.ds(kv_mine * core_id, kv_mine)]
    q_at = lambda ref, core_id: ref.at[:, :, core_id]

    ins = (
        (kv_in, kv_at, kvb.at[chip, :, 0, :, core]),
        (kv_in, lambda ref, core_id: kv_at(ref, core_id + 2), kvb.at[chip, :, 1, :, core]),
        (q_in, q_at, raw.at[0, :, core]),
        (g_in, q_at, raw.at[1, :, core]),
    )

    def in_local(n):
        src, at, dst = ins[n]
        return pltpu.make_async_copy(at(src, core), dst, in_loc.at[n])

    def in_remote(n):
        src, at, dst = ins[n]
        return pltpu.make_async_remote_copy(
            src_ref=at(src, other), dst_ref=dst, send_sem=in_send.at[n], recv_sem=in_recv.at[n],
            device_id={"ctx": partner}, device_id_type=MESH)

    def wait_in(n):
        in_local(n).wait()
        in_remote(n).wait()

    for n in range(4):
        in_local(n).start()

    barrier = pltpu.get_barrier_semaphore()
    for neighbour in (partner, up, down):
        pl.semaphore_signal(barrier, inc=1, device_id={"ctx": neighbour}, device_id_type=MESH)
    pl.semaphore_wait(barrier, 3)

    for n in range(4):
        in_remote(n).start()

    def ring_to(direction):
        return (me + n_dev + 2 - 4 * direction) % n_dev

    def ag_copy(b, h, direction, hop, kv):
        return pltpu.make_async_remote_copy(
            src_ref=kvb.at[b, h, kv], dst_ref=kvb.at[b, h, kv],
            send_sem=ag_send.at[direction, h, hop - 1, kv], recv_sem=ag_recv.at[direction, h, hop - 1, kv],
            device_id={"ctx": ring_to(direction)}, device_id_type=MESH)

    def chain_of(name):
        return {"A": (0, 0), "D": (0, 1), "C": (1, 0), "B": (1, 1)}[name]

    def pick(n, values):
        if len(set(values)) == 1:
            return values[0]
        total = 0
        for k, value in enumerate(values):
            if value:
                total = total + value * (n == k).astype(jnp.int32)
        return total

    def pick_item(n, names):
        chains = [chain_of(name[0]) for name in names]
        h = pick(n, [c[0] for c in chains])
        direction = pick(n, [c[1] for c in chains])
        return h, direction, pick(n, [int(name[1:]) for name in names])

    def owner(direction, d):
        return (chip + chips + (2 * direction - 1) * d) % chips

    def receive(*items):
        for kv in range(2):
            for h, direction, d in items:
                b = owner(direction, d)
                hops = half - (h + direction) % 2
                ag_copy(b, h, direction, d, kv).wait_recv()

                @pl.when(d < hops)
                def _():
                    ag_copy(b, h, direction, d + 1, kv).start()

    def send_own(name):
        for kv in range(2):
            ag_copy(chip, *chain_of(name), 1, kv).start()

    def named(name):
        return (*chain_of(name[0]), int(name[1:]))

    wait_in(0)
    wait_in(1)
    send_own("A")
    send_own("D")

    def init_body(n, carry):
        gi, qc = n // 4, n % 4
        ms[gi, qc] = jnp.full((1, piece), NEG, F32)
        ls[gi, qc] = jnp.zeros((1, piece), F32)
        oT[gi, qc] = jnp.zeros((dim, piece), F32)
        return carry

    lax.fori_loop(0, q_mine * 4, init_body, 0)

    def split_heads(n, dst):
        def body(c, carry):
            hi, co = c // 2, c % 2
            rawf[c] = raw[n, hi, co].astype(F32).reshape(piece * q_mine, dim)
            for gi in range(q_mine):
                dst[gi, hi, co] = rawf[c, pl.ds(gi, piece, stride=q_mine), :].astype(BF16)
            return carry

        wait_in(2 + n)
        lax.fori_loop(0, 4, body, 0)

    def join_heads(n):
        def body(c, carry):
            raw[n, c // 2, c % 2] = rawf[c].reshape(piece, q_mine, dim).astype(BF16)
            return carry

        lax.fori_loop(0, 4, body, 0)

    split_heads(0, qn)

    def visible(x, qc, width):
        k_idx = lax.broadcasted_iota(jnp.int32, (keys, width), 0)
        q_idx = lax.broadcasted_iota(jnp.int32, (keys, width), 1)
        if width > piece:
            q_idx = q_idx % piece
        in_high = (k_idx >= piece).astype(jnp.int32)
        k_pos = k_idx + x * (piece - keys * in_high)
        q_pos = q_idx + (piece * qc + x * (piece * (3 - 2 * qc)))
        return k_pos <= q_pos

    def fwd_step(b, h, x, qc, own):
        hi, co = qc // 2, qc % 2
        kk = kvb[b, h, 0, x].reshape(keys, dim)
        vv = kvb[b, h, 1, x].reshape(keys, dim)
        heads = [h * group + g for g in range(group)]
        q = jnp.concatenate([qn[gi, hi, co] for gi in heads], axis=0)
        s = dot_nt(kk, q)
        if own:
            s = jnp.where(visible(x, qc, group * piece), s, NEG)
        m0 = jnp.concatenate([ms[gi, qc] for gi in heads], axis=1)
        l0 = jnp.concatenate([ls[gi, qc] for gi in heads], axis=1)
        m1 = jnp.maximum(m0, jnp.max(s, axis=0, keepdims=True))
        p = jnp.exp2((s - m1) * cexp)
        decay = jnp.exp2((m0 - m1) * cexp)
        l1 = l0 * decay + jnp.sum(p, axis=0, keepdims=True)
        pv = dot(vv.T, p.astype(BF16))
        for g, gi in enumerate(heads):
            cols = slice(g * piece, (g + 1) * piece)
            ms[gi, qc] = m1[:, cols]
            ls[gi, qc] = l1[:, cols]
            oT[gi, qc] = oT[gi, qc] * decay[:, cols] + pv[:, cols]

    def bwd_step(b, h, x, qc, slot, own):
        hi, co = qc // 2, qc % 2
        kk = kvb[b, h, 0, x].reshape(keys, dim)
        vv = kvb[b, h, 1, x].reshape(keys, dim)
        k_t = kk.T
        mask = visible(x, qc, piece) if own else None
        dv = dk = None
        for g in range(group):
            gi = h * group + g
            q = qn[gi, hi, co]
            do = gn[gi, hi, co]
            s = dot_nt(kk, q)
            if own:
                s = jnp.where(mask, s, NEG)
            p = jnp.exp2(s * cexp - ms[gi, qc])
            dp = dot_nt(vv, do)
            ds = (p * (dp - ls[gi, qc])).astype(BF16)
            dv_part = dot(p.astype(BF16), do)
            dk_part = dot(ds, q)
            dv = dv_part if dv is None else dv + dv_part
            dk = dk_part if dk is None else dk + dk_part
            oT[gi, qc] += dot(k_t, ds)
        acc[slot, 0, x] += dk.reshape(2, piece, dim)
        acc[slot, 1, x] += dv.reshape(2, piece, dim)

    def far_steps(b, step):
        past = (b < chip).astype(jnp.int32)

        def body(w, carry):
            x = (1 - past) * (w // 2)
            qc = past * w + (1 - past) * (2 + w % 2)
            step(x, qc)
            return carry

        lax.fori_loop(0, 4, body, 0)

    def own_steps(step, start=0, stop=6):
        def body(n, carry):
            x = n // 4
            step(x, n - 2 * x)
            return carry

        lax.fori_loop(start, stop, body, 0)

    def own_fwd(h, start, stop):
        own_steps(lambda x, qc: fwd_step(chip, h, x, qc, True), start, stop)

    own_fwd(0, 0, 6)

    def fwd_far(h, direction, d):
        b = owner(direction, d)
        far_steps(b, lambda x, qc: fwd_step(b, h, x, qc, False))

    first = ["A1", "D1", "A2", "D2", "A3", "D3", "A4", "B1"]

    def fwd_pair(n, carry):
        receive(pick_item(n, first[0::2]), pick_item(n, first[1::2]))

        @pl.when(n == 1)
        def _():
            send_own("B")

        @pl.when(n == 2)
        def _():
            send_own("C")

        def one(k, inner):
            fwd_far(*pick_item(2 * n + k, first))
            return inner

        lax.fori_loop(0, 2 - n // 3, one, 0)

        @pl.when((n == 1) | (n == 2))
        def _():
            own_fwd(1, 3 * n - 3, 3 * n)

        return carry

    lax.fori_loop(0, 4, fwd_pair, 0)
    split_heads(1, gn)

    def fwd_end(h, qc, carry):
        hi, co = qc // 2, qc % 2
        for gi in range(h * group, (h + 1) * group):
            total = ls[gi, qc]
            o_t = oT[gi, qc] * (1.0 / total)
            rawf[qc, pl.ds(gi, piece, stride=q_mine), :] = o_t.T
            do_t = gn[gi, hi, co].astype(F32).T
            ls[gi, qc] = jnp.sum(o_t.astype(BF16).astype(F32) * do_t, axis=0, keepdims=True)
            ms[gi, qc] = ms[gi, qc] * cexp + jnp.log(total) * math.log2(math.e)
            oT[gi, qc] = jnp.zeros((dim, piece), F32)
        return carry

    lax.fori_loop(0, 4, functools.partial(fwd_end, 0), 0)

    outs = (
        (o_out, q_at, lambda k: raw.at[0, :, k]),
        (dq_out, q_at, lambda k: raw.at[1, :, k]),
        (dk_out, kv_at, lambda k: dkb.at[0, :, :, k]),
        (dv_out, kv_at, lambda k: dkb.at[1, :, :, k]),
    )

    def out_copies(n):
        dst, at, src = outs[n]
        local = pltpu.make_async_copy(src(core), at(dst, core), out_loc.at[n])
        remote = pltpu.make_async_remote_copy(
            src_ref=src(other), dst_ref=at(dst, core), send_sem=out_send.at[n], recv_sem=out_recv.at[n],
            device_id={"ctx": partner}, device_id_type=MESH)
        return local, remote

    def start_out(n):
        local, remote = out_copies(n)
        local.start()
        remote.start()

    def rs_copy(b, h, direction, d, slot, kv):
        return pltpu.make_async_remote_copy(
            src_ref=rbuf.at[b, h, kv], dst_ref=rbuf.at[slot, h, kv],
            send_sem=rs_send.at[direction, h, d - 1, kv], recv_sem=rs_recv.at[direction, h, d - 1, kv],
            device_id={"ctx": ring_to(1 - direction)}, device_id_type=MESH)

    def rs_send_copy(h, direction, d, kv):
        b = owner(direction, d)
        last = jnp.asarray(d == 1).astype(jnp.int32)
        return rs_copy(b, h, direction, d, b + last * direction * (chips - b), kv)

    def bwd_far(h, direction, d, slot):
        b = owner(direction, d)
        acc[slot] = jnp.zeros(acc.shape[1:], F32)
        far_steps(b, lambda x, qc: bwd_step(b, h, x, qc, slot, False))

    def rs_first(h, direction, d):
        for kv in range(2):
            rs_send_copy(h, direction, d, kv).start()

    def rs_next(h, direction, d, slot, kv):
        b = owner(direction, d)
        rs_copy(b, h, direction, d + 1, b, kv).wait_recv()
        rbuf[b, h, kv] += acc[slot, kv]
        rs_send_copy(h, direction, d, kv).start()

    early = ["A4", "D3"]

    def early_item(n, carry):
        h, direction, d = pick_item(n, early)
        bwd_far(h, direction, d, kv_mine)
        rbuf[owner(direction, d), h] = acc[kv_mine]

        @pl.when(n == 0)
        def _():
            receive(named("C1"), named("B2"))

        return carry

    lax.fori_loop(0, 2, early_item, 0)

    second = ["B1", "C1", "B2", "C2", "B3", "C3", "B4"]

    def fwd_late(n, carry):
        @pl.when(n == 1)
        def _():
            receive(named("C2"), named("B3"))
            for name in early:
                rs_first(*named(name))

        @pl.when(n == 5)
        def _():
            receive(named("C3"), named("B4"))

        fwd_far(*pick_item(n, second))
        return carry

    lax.fori_loop(0, len(second), fwd_late, 0)
    lax.fori_loop(0, 4, functools.partial(fwd_end, 1), 0)
    late = ["C3", "B4", "A3", "D2", "C2", "B3", "A2", "D1", "C1", "B2"]
    final = ["A1", "B1"]

    def own_bwd(h):
        acc[h] = jnp.zeros(acc.shape[1:], F32)
        own_steps(lambda x, qc: bwd_step(chip, h, x, qc, h, True))

    def late_item(n, carry):
        @pl.when((n == 6) | (n == 8))
        def _():
            own_bwd((n - 6) // 2)

        @pl.when(n == 2)
        def _():
            join_heads(0)
            start_out(0)

        which = pick_item(n, late + final)
        bwd_far(*which, kv_mine + n // 11)

        @pl.when(n < 2)
        def _():
            h, direction, d = which
            rbuf[owner(direction, d), h] = acc[kv_mine]
            rs_first(*which)

        @pl.when((n >= 2) & (n < 10))
        def _():
            for kv in range(2):
                rs_next(*which, kv_mine, kv)

        return carry

    lax.fori_loop(0, 12, late_item, 0)

    def wait_out(n):
        local, remote = out_copies(n)
        local.wait()
        remote.wait()

    def dq_end(qc, carry):
        for gi in range(q_mine):
            rawf[qc, pl.ds(gi, piece, stride=q_mine), :] = (oT[gi, qc] * scale).T
        return carry

    lax.fori_loop(0, 4, dq_end, 0)
    join_heads(1)
    start_out(1)

    for kv in range(2):
        for n, name in enumerate(final):
            rs_next(*named(name), kv_mine + n, kv)

    for kv in range(2):
        def kv_end(h, carry):
            for direction in range(2):
                rs_copy(chip, h, direction, 1, chip, kv).wait_recv()
            total = acc[h, kv] + rbuf[chip, h, kv] + rbuf[chips, h, kv]
            dkb[kv, h] = (total * scale if kv == 0 else total).astype(BF16)
            return carry

        lax.fori_loop(0, kv_mine, kv_end, 0)
        start_out(2 + kv)

    def drain(n, carry):
        h, direction = n % 2, n // 2
        hops = half - (h + direction) % 2

        def one(d, inner):
            for kv in range(2):
                rs_send_copy(h, direction, d, kv).wait_send()
                ag_copy(owner(direction, d - 1), h, direction, d, kv).wait_send()
            return inner

        lax.fori_loop(1, hops + 1, one, 0)
        return carry

    lax.fori_loop(0, 4, drain, 0)
    for n in range(4):
        wait_out(n)


def solution(mesh):
    chips = mesh.shape["ctx"] // 2
    block_spec = P("data", "ctx", None, None)

    def heads_first(x):
        _, tokens, heads, dim = x.shape
        return jnp.transpose(x[0], (1, 0, 2)).reshape(heads, 2, tokens // 2, dim)

    def token_rows(x):
        _, tokens, heads, dim = x.shape
        return x.reshape(2, tokens // 2, 2, heads // 2, dim)

    def tokens_first(x, like):
        _, tokens, heads, dim = like.shape
        return jnp.transpose(x.reshape(heads, tokens, dim), (1, 0, 2))[None]

    def local_attention(queries, keys_in, values_in, grad_out):
        _, tokens, q_heads, dim = queries.shape
        kv_heads = keys_in.shape[2]
        piece = tokens // 2
        q_mine, kv_mine = q_heads // 2, kv_heads // 2
        half = chips // 2
        dma = pltpu.SemaphoreType.DMA
        q_shape = jax.ShapeDtypeStruct((2, piece, 2, q_mine, dim), BF16)
        kv_shape = jax.ShapeDtypeStruct((kv_heads, 2, piece, dim), BF16)
        any_spec = pl.BlockSpec(memory_space=pl.ANY)
        outs = pl.pallas_call(
            functools.partial(attention_kernel, chips),
            out_shape=(q_shape, q_shape, kv_shape, kv_shape),
            in_specs=[any_spec] * 3,
            out_specs=(any_spec,) * 4,
            scratch_shapes=[
                pltpu.VMEM((q_mine, 2, 2, piece, dim), BF16),
                pltpu.VMEM((q_mine, 2, 2, piece, dim), BF16),
                pltpu.VMEM((chips, kv_mine, 2, 2, 2, piece, dim), BF16),
                pltpu.VMEM((q_mine, 4, dim, piece), F32),
                pltpu.VMEM((q_mine, 4, 1, piece), F32),
                pltpu.VMEM((q_mine, 4, 1, piece), F32),
                pltpu.VMEM((2, 2, 2, piece, q_mine, dim), BF16),
                pltpu.VMEM((4, piece * q_mine, dim), F32),
                pltpu.VMEM((chips + 1, kv_mine, 2, 2, 2, piece, dim), F32),
                pltpu.VMEM((kv_mine + 2, 2, 2, 2, piece, dim), F32),
                pltpu.VMEM((2, kv_mine, 2, 2, piece, dim), BF16),
                dma((4,)), dma((4,)), dma((4,)),
                dma((2, kv_mine, half, 2)), dma((2, kv_mine, half, 2)),
                dma((2, kv_mine, half, 2)), dma((2, kv_mine, half, 2)),
                dma((4,)), dma((4,)), dma((4,)),
            ],
            compiler_params=pltpu.CompilerParams(
                collective_id=0, has_side_effects=True, vmem_limit_bytes=60 * 2**20),
            name="ring_attention",
        )(token_rows(queries), heads_first(jnp.concatenate([keys_in, values_in], axis=2)), token_rows(grad_out))
        return (outs[0].reshape(queries.shape), outs[1].reshape(queries.shape),
                tokens_first(outs[2], keys_in), tokens_first(outs[3], keys_in))

    return jax.shard_map(local_attention, mesh=mesh, in_specs=(block_spec,) * 4, out_specs=(block_spec,) * 4, check_vma=False)
```

```python
import functools
import math

import jax
import jax.numpy as jnp
from jax import lax
from jax.experimental import pallas as pl
from jax.experimental.pallas import tpu as pltpu
from jax.sharding import PartitionSpec as P

F32 = jnp.float32
BF16 = jnp.bfloat16
NEG = -1e30
MESH = pl.DeviceIdType.MESH
NT_DIMS = (((1,), (1,)), ((), ()))


def dot(a, b):
    return jnp.dot(a, b, preferred_element_type=F32)


def dot_nt(a, b):
    return lax.dot_general(a, b, NT_DIMS, preferred_element_type=F32)


def attention_kernel(
    chips, q_in, kv_in, g_in, o_out, dq_out, dk_out, dv_out,
    qn, gn, kvb, oT, ms, ls, raw, rawf, rbuf, acc, dkb,
    in_loc, in_send, in_recv, ag_send, ag_recv, rs_send, rs_recv, out_loc, out_send, out_recv,
):
    q_mine = qn.shape[0]
    piece, dim = qn.shape[3], qn.shape[4]
    kv_mine = kvb.shape[1]
    group = q_mine // kv_mine
    half = chips // 2
    scale = dim ** -0.5
    cexp = scale * math.log2(math.e)
    keys = 2 * piece

    me = lax.axis_index("ctx")
    core = me % 2
    chip = me // 2
    other = 1 - core
    n_dev = 2 * chips
    partner = me + 1 - 2 * core
    up = (me + 2) % n_dev
    down = (me + n_dev - 2) % n_dev

    kv_at = lambda ref, core_id: ref.at[pl.ds(kv_mine * core_id, kv_mine)]
    q_at = lambda ref, core_id: ref.at[:, :, core_id]

    ins = (
        (kv_in, kv_at, kvb.at[chip, :, 0, :, core]),
        (kv_in, lambda ref, core_id: kv_at(ref, core_id + 2), kvb.at[chip, :, 1, :, core]),
        (q_in, q_at, raw.at[0, :, core]),
        (g_in, q_at, raw.at[1, :, core]),
    )

    def in_local(n):
        src, at, dst = ins[n]
        return pltpu.make_async_copy(at(src, core), dst, in_loc.at[n])

    def in_remote(n):
        src, at, dst = ins[n]
        return pltpu.make_async_remote_copy(
            src_ref=at(src, other), dst_ref=dst, send_sem=in_send.at[n], recv_sem=in_recv.at[n],
            device_id={"ctx": partner}, device_id_type=MESH)

    def wait_in(n):
        in_local(n).wait()
        in_remote(n).wait()

    for n in range(4):
        in_local(n).start()

    barrier = pltpu.get_barrier_semaphore()
    for neighbour in (partner, up, down):
        pl.semaphore_signal(barrier, inc=1, device_id={"ctx": neighbour}, device_id_type=MESH)
    pl.semaphore_wait(barrier, 3)

    for n in range(4):
        in_remote(n).start()

    def ring_to(direction):
        return (me + n_dev + 2 - 4 * direction) % n_dev

    def ag_copy(b, h, direction, hop, kv):
        return pltpu.make_async_remote_copy(
            src_ref=kvb.at[b, h, kv], dst_ref=kvb.at[b, h, kv],
            send_sem=ag_send.at[direction, h, hop - 1, kv], recv_sem=ag_recv.at[direction, h, hop - 1, kv],
            device_id={"ctx": ring_to(direction)}, device_id_type=MESH)

    def chain_of(name):
        return {"A": (0, 0), "D": (0, 1), "C": (1, 0), "B": (1, 1)}[name]

    def pick(n, values):
        if len(set(values)) == 1:
            return values[0]
        if isinstance(n, int):
            return values[n]
        total = 0
        for k, value in enumerate(values):
            if value:
                total = total + value * (n == k).astype(jnp.int32)
        return total

    def pick_item(n, names):
        chains = [chain_of(name[0]) for name in names]
        h = pick(n, [c[0] for c in chains])
        direction = pick(n, [c[1] for c in chains])
        return h, direction, pick(n, [int(name[1:]) for name in names])

    def owner(direction, d):
        return (chip + chips + (2 * direction - 1) * d) % chips

    def receive(*items, parts=(0, 1)):
        for kv in parts:
            for h, direction, d in items:
                b = owner(direction, d)
                hops = half - (h + direction) % 2
                ag_copy(b, h, direction, d, kv).wait_recv()

                @pl.when(d < hops)
                def _():
                    ag_copy(b, h, direction, d + 1, kv).start()

    def send_own(name):
        for kv in range(2):
            ag_copy(chip, *chain_of(name), 1, kv).start()

    def named(name):
        return (*chain_of(name[0]), int(name[1:]))

    wait_in(0)
    wait_in(1)
    send_own("A")
    send_own("D")

    def init_body(n, carry):
        gi, qc = n // 4, n % 4
        ms[gi, qc] = jnp.full((1, piece), NEG, F32)
        ls[gi, qc] = jnp.zeros((1, piece), F32)
        oT[gi, qc] = jnp.zeros((dim, piece), F32)
        return carry

    lax.fori_loop(0, q_mine * 4, init_body, 0)

    def split_heads(n, dst):
        def body(c, carry):
            hi, co = c // 2, c % 2
            rawf[c] = raw[n, hi, co].astype(F32).reshape(piece * q_mine, dim)
            for gi in range(q_mine):
                dst[gi, hi, co] = rawf[c, pl.ds(gi, piece, stride=q_mine), :].astype(BF16)
            return carry

        wait_in(2 + n)
        lax.fori_loop(0, 4, body, 0)

    def join_heads(n):
        def body(c, carry):
            raw[n, c // 2, c % 2] = rawf[c].reshape(piece, q_mine, dim).astype(BF16)
            return carry

        lax.fori_loop(0, 4, body, 0)

    split_heads(0, qn)

    def visible(x, qc, width):
        k_idx = lax.broadcasted_iota(jnp.int32, (keys, width), 0)
        q_idx = lax.broadcasted_iota(jnp.int32, (keys, width), 1)
        if width > piece:
            q_idx = q_idx % piece
        in_high = (k_idx >= piece).astype(jnp.int32)
        k_pos = k_idx + x * (piece - keys * in_high)
        q_pos = q_idx + (piece * qc + x * (piece * (3 - 2 * qc)))
        return k_pos <= q_pos

    def fwd_step(b, h, x, qc, own):
        hi, co = qc // 2, qc % 2
        kk = kvb[b, h, 0, x].reshape(keys, dim)
        vv = kvb[b, h, 1, x].reshape(keys, dim)
        heads = [h * group + g for g in range(group)]
        q = jnp.concatenate([qn[gi, hi, co] for gi in heads], axis=0)
        s = dot_nt(kk, q)
        if own:
            s = jnp.where(visible(x, qc, group * piece), s, NEG)
        m0 = jnp.concatenate([ms[gi, qc] for gi in heads], axis=1)
        l0 = jnp.concatenate([ls[gi, qc] for gi in heads], axis=1)
        m1 = jnp.maximum(m0, jnp.max(s, axis=0, keepdims=True))
        p = jnp.exp2((s - m1) * cexp)
        decay = jnp.exp2((m0 - m1) * cexp)
        l1 = l0 * decay + jnp.sum(p, axis=0, keepdims=True)
        pv = dot(vv.T, p.astype(BF16))
        for g, gi in enumerate(heads):
            cols = slice(g * piece, (g + 1) * piece)
            ms[gi, qc] = m1[:, cols]
            ls[gi, qc] = l1[:, cols]
            oT[gi, qc] = oT[gi, qc] * decay[:, cols] + pv[:, cols]

    def bwd_step(b, h, x, qc, slot, own):
        hi, co = qc // 2, qc % 2
        kk = kvb[b, h, 0, x].reshape(keys, dim)
        vv = kvb[b, h, 1, x].reshape(keys, dim)
        k_t = kk.T
        mask = visible(x, qc, piece) if own else None
        dv = dk = None
        for g in range(group):
            gi = h * group + g
            q = qn[gi, hi, co]
            do = gn[gi, hi, co]
            s = dot_nt(kk, q)
            if own:
                s = jnp.where(mask, s, NEG)
            p = jnp.exp2(s * cexp - ms[gi, qc])
            dp = dot_nt(vv, do)
            ds = (p * (dp - ls[gi, qc])).astype(BF16)
            dv_part = dot(p.astype(BF16), do)
            dk_part = dot(ds, q)
            dv = dv_part if dv is None else dv + dv_part
            dk = dk_part if dk is None else dk + dk_part
            oT[gi, qc] += dot(k_t, ds)
        acc[slot, 0, x] += dk.reshape(2, piece, dim)
        acc[slot, 1, x] += dv.reshape(2, piece, dim)

    def far_steps(b, step):
        past = (b < chip).astype(jnp.int32)

        def body(w, carry):
            x = (1 - past) * (w // 2)
            qc = past * w + (1 - past) * (2 + w % 2)
            step(x, qc)
            return carry

        lax.fori_loop(0, 4, body, 0)

    def own_steps(step, start=0, stop=6):
        def body(n, carry):
            x = n // 4
            step(x, n - 2 * x)
            return carry

        lax.fori_loop(start, stop, body, 0)

    def own_fwd(h, start, stop):
        own_steps(lambda x, qc: fwd_step(chip, h, x, qc, True), start, stop)

    own_fwd(0, 0, 6)

    def fwd_far(h, direction, d):
        b = owner(direction, d)
        far_steps(b, lambda x, qc: fwd_step(b, h, x, qc, False))

    first = ["A1", "D1", "A2", "D2", "A3", "D3", "A4", "B1"]

    def receive_pair(n, part):
        receive(pick_item(n, first[0::2]), pick_item(n, first[1::2]), parts=(part,))

    def fwd_pair(n, carry):
        receive_pair(n, 1)

        @pl.when(n == 1)
        def _():
            send_own("B")

        @pl.when(n == 2)
        def _():
            send_own("C")

        def one(k, inner):
            fwd_far(*pick_item(2 * n + k, first))
            return inner

        lax.fori_loop(0, 2 - n // 3, one, 0)

        @pl.when(n < 3)
        def _():
            receive_pair(n + 1, 0)

        @pl.when((n == 1) | (n == 2))
        def _():
            own_fwd(1, 3 * n - 3, 3 * n)

        return carry

    receive_pair(0, 0)
    lax.fori_loop(0, 4, fwd_pair, 0)
    split_heads(1, gn)

    def fwd_end(h, qc, carry):
        hi, co = qc // 2, qc % 2
        for gi in range(h * group, (h + 1) * group):
            total = ls[gi, qc]
            o_t = oT[gi, qc] * (1.0 / total)
            rawf[qc, pl.ds(gi, piece, stride=q_mine), :] = o_t.T
            do_t = gn[gi, hi, co].astype(F32).T
            ls[gi, qc] = jnp.sum(o_t.astype(BF16).astype(F32) * do_t, axis=0, keepdims=True)
            ms[gi, qc] = ms[gi, qc] * cexp + jnp.log(total) * math.log2(math.e)
            oT[gi, qc] = jnp.zeros((dim, piece), F32)
        return carry

    lax.fori_loop(0, 4, functools.partial(fwd_end, 0), 0)

    outs = (
        (o_out, q_at, lambda k: raw.at[0, :, k]),
        (dq_out, q_at, lambda k: raw.at[1, :, k]),
        (dk_out, kv_at, lambda k: dkb.at[0, :, :, k]),
        (dv_out, kv_at, lambda k: dkb.at[1, :, :, k]),
    )

    def out_copies(n):
        dst, at, src = outs[n]
        local = pltpu.make_async_copy(src(core), at(dst, core), out_loc.at[n])
        remote = pltpu.make_async_remote_copy(
            src_ref=src(other), dst_ref=at(dst, core), send_sem=out_send.at[n], recv_sem=out_recv.at[n],
            device_id={"ctx": partner}, device_id_type=MESH)
        return local, remote

    def start_out(n):
        local, remote = out_copies(n)
        local.start()
        remote.start()

    def rs_copy(b, h, direction, d, slot, kv):
        return pltpu.make_async_remote_copy(
            src_ref=rbuf.at[b, h, kv], dst_ref=rbuf.at[slot, h, kv],
            send_sem=rs_send.at[direction, h, d - 1, kv], recv_sem=rs_recv.at[direction, h, d - 1, kv],
            device_id={"ctx": ring_to(1 - direction)}, device_id_type=MESH)

    def rs_send_copy(h, direction, d, kv):
        b = owner(direction, d)
        last = jnp.asarray(d == 1).astype(jnp.int32)
        return rs_copy(b, h, direction, d, b + last * direction * (chips - b), kv)

    def bwd_far(h, direction, d, slot):
        b = owner(direction, d)
        acc[slot] = jnp.zeros(acc.shape[1:], F32)
        far_steps(b, lambda x, qc: bwd_step(b, h, x, qc, slot, False))

    def rs_first(h, direction, d):
        for kv in range(2):
            rs_send_copy(h, direction, d, kv).start()

    def rs_next(h, direction, d, slot, kv):
        b = owner(direction, d)
        rs_copy(b, h, direction, d + 1, b, kv).wait_recv()
        rbuf[b, h, kv] += acc[slot, kv]
        rs_send_copy(h, direction, d, kv).start()

    early = ["A4", "D3"]

    def early_item(n, carry):
        h, direction, d = pick_item(n, early)
        bwd_far(h, direction, d, kv_mine)
        rbuf[owner(direction, d), h] = acc[kv_mine]

        @pl.when(n == 0)
        def _():
            receive(named("C1"), named("B2"), parts=(1,))

        return carry

    receive(named("C1"), named("B2"), parts=(0,))
    lax.fori_loop(0, 2, early_item, 0)
    receive(named("C2"), named("B3"), parts=(0,))

    second = ["B1", "C1", "B2", "C2", "B3", "C3", "B4"]

    def fwd_late(n, carry):
        @pl.when(n == 1)
        def _():
            receive(named("C2"), named("B3"), parts=(1,))
            for name in early:
                rs_first(*named(name))

        @pl.when(n == 5)
        def _():
            receive(named("C3"), named("B4"))

        fwd_far(*pick_item(n, second))
        return carry

    lax.fori_loop(0, len(second), fwd_late, 0)
    lax.fori_loop(0, 4, functools.partial(fwd_end, 1), 0)
    late = ["C3", "B4", "A3", "D2", "C2", "B3", "A2", "D1", "C1", "B2"]
    final = ["A1", "B1"]

    def own_bwd(h):
        acc[h] = jnp.zeros(acc.shape[1:], F32)
        own_steps(lambda x, qc: bwd_step(chip, h, x, qc, h, True))

    def late_item(n, carry):
        @pl.when((n == 6) | (n == 8))
        def _():
            own_bwd((n - 6) // 2)

        @pl.when(n == 2)
        def _():
            join_heads(0)
            start_out(0)

        which = pick_item(n, late + final)
        bwd_far(*which, kv_mine + n // 11)

        @pl.when(n < 2)
        def _():
            h, direction, d = which
            rbuf[owner(direction, d), h] = acc[kv_mine]
            rs_first(*which)

        @pl.when((n >= 2) & (n < 10))
        def _():
            for kv in range(2):
                rs_next(*which, kv_mine, kv)

        return carry

    lax.fori_loop(0, 12, late_item, 0)

    def wait_out(n):
        local, remote = out_copies(n)
        local.wait()
        remote.wait()

    def dq_end(qc, carry):
        for gi in range(q_mine):
            rawf[qc, pl.ds(gi, piece, stride=q_mine), :] = (oT[gi, qc] * scale).T
        return carry

    lax.fori_loop(0, 4, dq_end, 0)
    join_heads(1)
    start_out(1)

    for kv in range(2):
        for n, name in enumerate(final):
            rs_next(*named(name), kv_mine + n, kv)

    for kv in range(2):
        def kv_end(h, carry):
            for direction in range(2):
                rs_copy(chip, h, direction, 1, chip, kv).wait_recv()
            total = acc[h, kv] + rbuf[chip, h, kv] + rbuf[chips, h, kv]
            dkb[kv, h] = (total * scale if kv == 0 else total).astype(BF16)
            return carry

        lax.fori_loop(0, kv_mine, kv_end, 0)
        start_out(2 + kv)

    def drain(n, carry):
        h, direction = n % 2, n // 2
        hops = half - (h + direction) % 2

        def one(d, inner):
            for kv in range(2):
                rs_send_copy(h, direction, d, kv).wait_send()
                ag_copy(owner(direction, d - 1), h, direction, d, kv).wait_send()
            return inner

        lax.fori_loop(1, hops + 1, one, 0)
        return carry

    lax.fori_loop(0, 4, drain, 0)
    for n in range(4):
        wait_out(n)


def solution(mesh):
    chips = mesh.shape["ctx"] // 2
    block_spec = P("data", "ctx", None, None)

    def heads_first(x):
        _, tokens, heads, dim = x.shape
        return jnp.transpose(x[0], (1, 0, 2)).reshape(heads, 2, tokens // 2, dim)

    def token_rows(x):
        _, tokens, heads, dim = x.shape
        return x.reshape(2, tokens // 2, 2, heads // 2, dim)

    def tokens_first(x, like):
        _, tokens, heads, dim = like.shape
        return jnp.transpose(x.reshape(heads, tokens, dim), (1, 0, 2))[None]

    def local_attention(queries, keys_in, values_in, grad_out):
        _, tokens, q_heads, dim = queries.shape
        kv_heads = keys_in.shape[2]
        piece = tokens // 2
        q_mine, kv_mine = q_heads // 2, kv_heads // 2
        half = chips // 2
        dma = pltpu.SemaphoreType.DMA
        q_shape = jax.ShapeDtypeStruct((2, piece, 2, q_mine, dim), BF16)
        kv_shape = jax.ShapeDtypeStruct((kv_heads, 2, piece, dim), BF16)
        any_spec = pl.BlockSpec(memory_space=pl.ANY)
        outs = pl.pallas_call(
            functools.partial(attention_kernel, chips),
            out_shape=(q_shape, q_shape, kv_shape, kv_shape),
            in_specs=[any_spec] * 3,
            out_specs=(any_spec,) * 4,
            scratch_shapes=[
                pltpu.VMEM((q_mine, 2, 2, piece, dim), BF16),
                pltpu.VMEM((q_mine, 2, 2, piece, dim), BF16),
                pltpu.VMEM((chips, kv_mine, 2, 2, 2, piece, dim), BF16),
                pltpu.VMEM((q_mine, 4, dim, piece), F32),
                pltpu.VMEM((q_mine, 4, 1, piece), F32),
                pltpu.VMEM((q_mine, 4, 1, piece), F32),
                pltpu.VMEM((2, 2, 2, piece, q_mine, dim), BF16),
                pltpu.VMEM((4, piece * q_mine, dim), F32),
                pltpu.VMEM((chips + 1, kv_mine, 2, 2, 2, piece, dim), F32),
                pltpu.VMEM((kv_mine + 2, 2, 2, 2, piece, dim), F32),
                pltpu.VMEM((2, kv_mine, 2, 2, piece, dim), BF16),
                dma((4,)), dma((4,)), dma((4,)),
                dma((2, kv_mine, half, 2)), dma((2, kv_mine, half, 2)),
                dma((2, kv_mine, half, 2)), dma((2, kv_mine, half, 2)),
                dma((4,)), dma((4,)), dma((4,)),
            ],
            compiler_params=pltpu.CompilerParams(
                collective_id=0, has_side_effects=True, vmem_limit_bytes=60 * 2**20),
            name="ring_attention",
        )(token_rows(queries), heads_first(jnp.concatenate([keys_in, values_in], axis=2)), token_rows(grad_out))
        return (outs[0].reshape(queries.shape), outs[1].reshape(queries.shape),
                tokens_first(outs[2], keys_in), tokens_first(outs[3], keys_in))

    return jax.shard_map(local_attention, mesh=mesh, in_specs=(block_spec,) * 4, out_specs=(block_spec,) * 4, check_vma=False)
```
